32 devices in a mesh: grp: 4 (over y, x), zero: 8 (over z, core).
Axes of the slice: x: 2, y: 2, z: 4, core: 2. Of those that a mesh axis runs over, the one named last changes fastest.
Arguments:
- replica_grads: bfloat16 [4, 3072, 2, 12288], P('grp', None, None, 'zero'), may hold values from -20000 to 20000, as said below
- master_weights: float32 [3072, 2, 12288], P(('grp', 'zero')), may hold values from -0.6 to 0.6
- first_moment: float32 [3072, 2, 12288], P(('grp', 'zero')), may hold values from -0.3 to 0.3
- second_moment: float32 [3072, 2, 12288], P(('grp', 'zero')), may hold values from 0.001 to 0.03
- max_norm: float32 [1], replicated, may hold values from 1737.7856 to 4344.464
Outputs:
- new_master: float32 [3072, 2, 12288], P(('grp', 'zero'))
- new_first: float32 [3072, 2, 12288], P(('grp', 'zero'))
- new_second: float32 [3072, 2, 12288], P(('grp', 'zero'))
- new_weights: bfloat16 [3072, 2, 12288], P(None, None, 'zero')
The draws below stay inside these ranges and needn't reach their ends.
Inputs may be any that keep to these rules, and one draw needn't show every extreme that they name: `replica_grads`: one gradient of the joined weight for each replica group.
All inputs are finite; a program needn't handle non-finite values.
Results may differ from the reference program's by a relative error of at most 0.015.
Values may be sent and summed in bfloat16 or wider, within the bound.
A program may use at most 192 MiB of HBM per device.

```python
import math
import jax
import jax.numpy as jnp

D = 3072
FF = 12288
ADAM_STEP = 10
N_GRP = 4


def draw_replica_grads(key, part):
    first_key, second_key, third_key, fourth_key, fifth_key = jax.random.split(key, 5)
    log_top = math.log(10.0)
    row_index = jnp.arange(D, dtype=jnp.float32)
    column_index = jnp.arange(FF, dtype=jnp.float32)
    row_scale = jnp.sqrt(1.0 + 2.0 * row_index / (D - 1)) * jnp.exp(jax.random.uniform(first_key, (D,), jnp.float32) * log_top)
    column_scale = jnp.sqrt(1.0 + 2.0 * column_index / (FF - 1))[None, :] * jnp.exp(jax.random.uniform(second_key, (2, FF), jnp.float32) * log_top)
    levels = jnp.arange(N_GRP, dtype=jnp.float32) / max(N_GRP - 1, 1)
    band_mix = jax.random.permutation(fifth_key, levels)
    row_mix = jnp.repeat(band_mix, D // N_GRP, total_repeat_length=D)
    replica_sign = jnp.where(jnp.arange(N_GRP) % 2 == 0, 1.0, -1.0).astype(jnp.float32)
    common_weight = row_mix[None, :] + (1.0 - row_mix[None, :]) * replica_sign[:, None]
    independent = jax.random.truncated_normal(third_key, -4.0, 4.0, (N_GRP, D, 2, FF), jnp.float32)
    common = jax.random.truncated_normal(fourth_key, -4.0, 4.0, (D, 2, FF), jnp.float32)
    random_part = 0.5 * independent + common_weight[:, :, None, None] * common[None]
    values = random_part * row_scale[None, :, None, None] * column_scale[None, None, :, :]
    return values.astype(jnp.bfloat16)


def level_of(rng, shape, pieces, low, top_value):
    factor_of = 1.0
    for dim, blocks in pieces:
        steps = jax.random.uniform(jax.random.fold_in(jax.random.fold_in(rng, 6), dim), (blocks,), jnp.float32, low / len(pieces), top_value / len(pieces))
        factor_of = factor_of * jnp.repeat(jnp.exp(steps), shape[dim] // blocks).reshape((-1,) + (1,) * (len(shape) - 1 - dim))
    return factor_of


def gaussian(key, shape, scale, bound, cuts=(), held_as=jnp.bfloat16):
    values = scale * jax.random.normal(key, shape, jnp.float32)
    if cuts:
        values = values * level_of(key, shape, cuts, -0.22, 0.18)
    return jnp.clip(values, -bound, bound).astype(held_as)


def setup_inputs(seed: int = 0) -> dict:
    splits = jax.random.split(jax.random.key(seed), 6)
    return {
        "replica_grads": draw_replica_grads(jax.random.fold_in(splits[5], 71), 0),
        "master_weights": gaussian(splits[1], (D, 2, FF), 0.1, 0.6, ((0, 32),), jnp.float32),
        "first_moment": gaussian(splits[2], (D, 2, FF), 0.05, 0.3, ((0, 32),), jnp.float32),
        "second_moment": jnp.clip(jnp.exp(math.log(0.03) - 3.4011973 * jax.random.uniform(splits[3], (D, 2, FF), jnp.float32) ** level_of(splits[3], (D, 2, FF), ((0, 32),), -0.2, 0.2)), 0.001, 0.03),
        "max_norm": jnp.clip(jax.random.uniform(splits[4], (1,), jnp.float32, 1737.7856, 4344.464), 1737.7856, 4344.464),
    }


beta_one = 0.9
beta_two = 0.95
learn_rate = 0.02
adam_eps = 1e-08
norm_eps = 1e-06

def adam_update(summed, master, first, second, scale):
    clipped = summed * scale
    new_first = beta_one * first + (1.0 - beta_one) * clipped
    new_second = beta_two * second + (1.0 - beta_two) * clipped * clipped
    correct_one = 1.0 - beta_one ** ADAM_STEP
    correct_two = 1.0 - beta_two ** ADAM_STEP
    step_size = new_first / correct_one / (jnp.sqrt(new_second / correct_two) + adam_eps)
    new_master = master - learn_rate * step_size
    return (new_master, new_first, new_second)

def reference(replica_grads, master_weights, first_moment, second_moment, max_norm):
    summed = replica_grads[0].astype(jnp.float32)
    for replica in range(1, N_GRP):
        summed = summed + replica_grads[replica].astype(jnp.float32)
    total = jnp.sum(summed * summed)
    scale = jnp.minimum(jnp.float32(1.0), max_norm[0] / (jnp.sqrt(total) + norm_eps))
    new_master, new_first, new_second = adam_update(summed, master_weights, first_moment, second_moment, scale)
    return (new_master, new_first, new_second, new_master.astype(jnp.bfloat16))
```

```python
import functools

import jax
import jax.numpy as jnp
from jax import lax
from jax.experimental import pallas as pl
from jax.experimental.pallas import tpu as pltpu
from jax.experimental.layout import Layout, with_layout_constraint
from jax.sharding import PartitionSpec as P

ADAM_STEP = 10
MESH = pl.DeviceIdType.MESH
LANES = 128

beta_one = 0.9
beta_two = 0.95
learn_rate = 0.02
adam_eps = 1e-08
norm_eps = 1e-06


def adam_update(summed, master, first, second, scale):
    clipped = summed * scale
    new_first = beta_one * first + (1.0 - beta_one) * clipped
    new_second = beta_two * second + (1.0 - beta_two) * clipped * clipped
    correct_one = 1.0 - beta_one**ADAM_STEP
    correct_two = 1.0 - beta_two**ADAM_STEP
    step_size = new_first / correct_one / (jnp.sqrt(new_second / correct_two) + adam_eps)
    new_master = master - learn_rate * step_size
    return (new_master, new_first, new_second)


def plain_body(replica_grads, master_weights, first_moment, second_moment, max_norm):
    groups = lax.axis_size("grp")
    shards = lax.axis_size("zero")
    local_grad = replica_grads[0]
    local_width = local_grad.shape[2]
    rows_dev = master_weights.shape[0]
    full_width = master_weights.shape[2]
    blocks = local_grad.reshape(groups, shards, rows_dev, 2, local_width)
    arrived = lax.all_to_all(
        lax.all_to_all(blocks[None], "grp", split_axis=1, concat_axis=0, tiled=True),
        "zero",
        split_axis=2,
        concat_axis=5,
        tiled=True,
    )
    summed = jnp.sum(arrived.astype(jnp.float32), axis=0)
    summed = summed.reshape(master_weights.shape)
    total = lax.psum(jnp.sum(summed * summed), ("grp", "zero"))
    scale = jnp.minimum(jnp.float32(1.0), max_norm[0] / (jnp.sqrt(total) + norm_eps))
    new_master, new_first, new_second = adam_update(
        summed, master_weights, first_moment, second_moment, scale
    )
    fresh = new_master.astype(jnp.bfloat16).reshape(1, 1, rows_dev, 2, full_width)
    own_tiles = lax.all_to_all(fresh, "zero", split_axis=4, concat_axis=1, tiled=True)
    tiled = lax.all_gather(own_tiles, "grp", axis=0, tiled=True)
    new_weights = tiled.reshape(groups * shards * rows_dev, 2, full_width // shards)
    return (new_master, new_first, new_second, new_weights)


def flip(index, mask, size):
    out = 0
    bit = 1
    while bit < size:
        b = (index // bit) % 2
        out = out + bit * ((1 - b) if mask & bit else b)
        bit *= 2
    return out


def greet(groups, shards, g, z):
    barrier = pltpu.get_barrier_semaphore()
    for k in range(1, shards):
        pl.semaphore_signal(barrier, inc=1, device_id=(g, flip(z, k, shards)), device_id_type=MESH)
    for j in range(1, groups):
        pl.semaphore_signal(barrier, inc=1, device_id=(flip(g, j, groups), z), device_id_type=MESH)
    pl.semaphore_wait(barrier, shards + groups - 2)


def remote(src, dst, send, recv, device):
    return pltpu.make_async_remote_copy(
        src_ref=src, dst_ref=dst, send_sem=send, recv_sem=recv,
        device_id=device, device_id_type=MESH,
    )


def scatter_kernel(groups, shards, grad, landed, norm, parts, own, sums, zone, gone,
                   p_send, p_recv, own_sem, s_send, s_recv, nz_send, nz_recv, ng_send, ng_recv, loc_sem):
    g, z = lax.axis_index("grp"), lax.axis_index("zero")
    rows = own.shape[1]
    order = list(range(shards - 1, -1, -1))

    def part(j, k):
        to = flip(g, j, groups)
        return remote(grad.at[to, flip(z, k, shards)], parts.at[j - 1, k],
                      p_send.at[j - 1, k], p_recv.at[j - 1, k], (to, z))

    def mine(k):
        return pltpu.make_async_copy(grad.at[g, flip(z, k, shards)], own.at[k], own_sem.at[k])

    def onward(k):
        return remote(sums.at[k], landed.at[z], s_send.at[k], s_recv.at[k], (g, flip(z, k, shards)))

    for k in order:
        mine(k).start()
    greet(groups, shards, g, z)
    for k in order:
        for j in range(1, groups):
            part(j, k).start()
    stay = pltpu.make_async_copy(sums.at[0], landed.at[z], loc_sem)
    square = jnp.zeros(own.shape[2:], jnp.float32)
    for k in order:
        mine(k).wait()
        for j in range(1, groups):
            part(j, k).wait_recv()

        def add(r, acc, k=k):
            total = own[k, r].astype(jnp.float32)
            for j in range(1, groups):
                total = total + parts[j - 1, k, r].astype(jnp.float32)
            sums[k, r] = total.astype(jnp.bfloat16)
            return acc + total * total

        square = lax.fori_loop(0, rows, add, square)
        if k:
            onward(k).start()
        else:
            stay.start()

    folded = square[0:8]
    for i in range(8, square.shape[0], 8):
        folded = folded + square[i:i + 8]
    zone[0] = folded

    def tell_zero(k):
        return remote(zone.at[0], zone.at[k], nz_send.at[k], nz_recv.at[k], (g, flip(z, k, shards)))

    def tell_group(j):
        return remote(gone.at[0], gone.at[j], ng_send.at[j], ng_recv.at[j], (flip(g, j, groups), z))

    for k in range(1, shards):
        tell_zero(k).start()
    for k in range(1, shards):
        tell_zero(k).wait_recv()
    gone[0] = jnp.sum(zone[...], axis=0)
    for j in range(1, groups):
        tell_group(j).start()
    for j in range(1, groups):
        tell_group(j).wait_recv()
    norm[...] = jnp.sum(gone[...], axis=0)

    for k in range(1, shards):
        tell_zero(k).wait_send()
    for j in range(1, groups):
        tell_group(j).wait_send()
    for k in order:
        for j in range(1, groups):
            part(j, k).wait_send()
        if k:
            onward(k).wait()
        else:
            stay.wait()


def update_kernel(limit, norm, summed, master, first, second, out_master, out_first, out_second, fresh):
    total = jnp.full(master.shape[2:], jnp.sum(norm[...]), jnp.float32)
    scale = jnp.minimum(jnp.float32(1.0), limit[0] / (jnp.sqrt(total) + norm_eps))

    def row(r, carry):
        for c in range(summed.shape[0]):
            new_master, new_first, new_second = adam_update(
                summed[c, r].astype(jnp.float32), master[r, c], first[r, c], second[r, c], scale
            )
            out_master[r, c] = new_master
            out_first[r, c] = new_first
            out_second[r, c] = new_second
            fresh[c, r] = new_master.astype(jnp.bfloat16)
        return carry

    lax.fori_loop(0, master.shape[0], row, 0)


def gather_kernel(groups, shards, fresh, out, hold, z_send, z_recv, x_send, x_recv, y_send, y_recv,
                  u_send, u_recv, v_send, v_recv, loc_sem):
    g, z = lax.axis_index("grp"), lax.axis_index("zero")
    half = fresh.shape[1] // 2
    gx, gy = flip(g, 1, groups), flip(g, 2, groups)

    def spread(k):
        return remote(fresh.at[flip(z, k, shards)], out.at[g, z], z_send.at[k], z_recv.at[k],
                      (g, flip(z, k, shards)))

    def first_hop(k, send, recv, to):
        q = flip(z, k, shards)
        src = out.at[g, q] if k else fresh.at[z]
        return remote(src, out.at[g, q], send.at[k], recv.at[k], (to, z))

    def second_hop(k, origin, start, send, recv, to):
        q = flip(z, k, shards)
        ref = out.at[origin, q, pl.ds(start, half)]
        return remote(ref, ref, send.at[k], recv.at[k], (to, z))

    def hops(k):
        return (first_hop(k, x_send, x_recv, gx), first_hop(k, y_send, y_recv, gy))

    def turns(k):
        return (second_hop(k, gx, 0, u_send, u_recv, gy), second_hop(k, gy, half, v_send, v_recv, gx))

    load = pltpu.make_async_copy(fresh.at[z], hold, loc_sem.at[0])
    store = pltpu.make_async_copy(hold, out.at[g, z], loc_sem.at[1])
    load.start()
    greet(groups, shards, g, z)
    for k in range(1, shards):
        spread(k).start()
    lag = 1
    for s in range(shards + lag):
        if s < shards:
            if s:
                spread(s).wait_recv()
            for hop in hops(s):
                hop.start()
            if s == 0:
                load.wait()
                store.start()
        if s >= lag:
            for hop, turn in zip(hops(s - lag), turns(s - lag)):
                hop.wait_recv()
                turn.start()
    store.wait()
    for k in range(shards):
        if k:
            spread(k).wait_send()
        for hop in hops(k):
            hop.wait_send()
        for turn in turns(k):
            turn.wait()


def flat_body(replica_grads, master_weights, first_moment, second_moment, max_norm):
    groups = lax.axis_size("grp")
    shards = lax.axis_size("zero")
    rows = master_weights.shape[0]
    width = replica_grads.shape[3]
    tiles = width // LANES
    deep = 2 * tiles
    bf16, f32 = jnp.bfloat16, jnp.float32
    any_space = pl.BlockSpec(memory_space=pl.ANY)
    dma = pltpu.SemaphoreType.DMA
    limit = 60 * 1024 * 1024

    def keep(x, *order):
        return with_layout_constraint(x, Layout(major_to_minor=order))

    def flat(x):
        x = x.reshape(x.shape[0], 2, -1, LANES)
        return jnp.swapaxes(keep(x, 0, 2, 1, 3), 1, 2)

    grad = flat(replica_grads[0]).reshape(groups, shards, rows, deep, LANES)
    master, first, second = (
        flat(x).reshape(rows, shards, deep, LANES)
        for x in (master_weights, first_moment, second_moment)
    )

    piece = (rows, deep, LANES)
    landed, norm = pl.pallas_call(
        functools.partial(scatter_kernel, groups, shards),
        out_shape=(
            jax.ShapeDtypeStruct((shards,) + piece, bf16),
            jax.ShapeDtypeStruct((8, LANES), f32),
        ),
        in_specs=[any_space],
        out_specs=(any_space, pl.BlockSpec(memory_space=pltpu.VMEM)),
        scratch_shapes=[
            pltpu.VMEM((groups - 1, shards) + piece, bf16),
            pltpu.VMEM((shards,) + piece, bf16),
            pltpu.VMEM((shards,) + piece, bf16),
            pltpu.VMEM((shards, 8, LANES), f32),
            pltpu.VMEM((groups, 8, LANES), f32),
            dma((groups - 1, shards)),
            dma((groups - 1, shards)),
            dma((shards,)),
            dma((shards,)),
            dma((shards,)),
            dma((shards,)),
            dma((shards,)),
            dma((groups,)),
            dma((groups,)),
            dma,
        ],
        compiler_params=pltpu.CompilerParams(
            collective_id=0, has_side_effects=True, vmem_limit_bytes=limit
        ),
    )(grad)

    step = 8 if rows % 8 == 0 else 1
    by_row = pl.BlockSpec((step, shards, deep, LANES), lambda i: (i, 0, 0, 0))
    by_shard = pl.BlockSpec((shards, step, deep, LANES), lambda i: (0, i, 0, 0))
    state = jax.ShapeDtypeStruct((rows, shards, deep, LANES), f32)
    new_master, new_first, new_second, fresh = pl.pallas_call(
        update_kernel,
        grid=(rows // step,),
        out_shape=(state, state, state, jax.ShapeDtypeStruct((shards,) + piece, bf16)),
        in_specs=[
            pl.BlockSpec(memory_space=pltpu.SMEM),
            pl.BlockSpec((8, LANES), lambda i: (0, 0)),
            by_shard, by_row, by_row, by_row,
        ],
        out_specs=(by_row, by_row, by_row, by_shard),
        compiler_params=pltpu.CompilerParams(vmem_limit_bytes=limit),
    )(max_norm, norm, landed, master, first, second)

    gathered = pl.pallas_call(
        functools.partial(gather_kernel, groups, shards),
        out_shape=jax.ShapeDtypeStruct((groups, shards) + piece, bf16),
        in_specs=[any_space],
        out_specs=any_space,
        scratch_shapes=[pltpu.VMEM(piece, bf16)] + [dma((shards,))] * 10 + [dma((2,))],
        compiler_params=pltpu.CompilerParams(
            collective_id=1, has_side_effects=True, vmem_limit_bytes=limit
        ),
    )(fresh)

    def unflat(x, shape):
        x = x.reshape(shape[0], -1, 2, LANES)
        return keep(jnp.swapaxes(x, 1, 2), 0, 2, 1, 3).reshape(shape)

    shape = master_weights.shape
    return (
        unflat(new_master, shape),
        unflat(new_first, shape),
        unflat(new_second, shape),
        unflat(gathered, replica_grads.shape[1:]),
    )


def body(replica_grads, master_weights, first_moment, second_moment, max_norm):
    groups = lax.axis_size("grp")
    shards = lax.axis_size("zero")
    rows = master_weights.shape[0]
    width = replica_grads.shape[3]
    deep = 2 * width // LANES
    power = shards > 1 and shards & (shards - 1) == 0
    fits = groups * shards * rows * deep * LANES * 2 * 3 // 2 < 48 * 1024 * 1024
    whole = width % LANES == 0 and deep % 8 == 0 and rows % 2 == 0
    run = flat_body if groups == 4 and power and fits and whole else plain_body
    return run(replica_grads, master_weights, first_moment, second_moment, max_norm)


def solution(mesh):
    in_specs = (
        P("grp", None, None, "zero"),
        P(("grp", "zero"), None, None),
        P(("grp", "zero"), None, None),
        P(("grp", "zero"), None, None),
        P(),
    )
    out_specs = (
        P(("grp", "zero"), None, None),
        P(("grp", "zero"), None, None),
        P(("grp", "zero"), None, None),
        P(None, None, "zero"),
    )
    return jax.shard_map(body, mesh=mesh, in_specs=in_specs, out_specs=out_specs, check_vma=False)
```

```python
import functools

import jax
import jax.numpy as jnp
from jax import lax
from jax.experimental import pallas as pl
from jax.experimental.pallas import tpu as pltpu
from jax.experimental.layout import Layout, with_layout_constraint
from jax.sharding import PartitionSpec as P

ADAM_STEP = 10
MESH = pl.DeviceIdType.MESH
LANES = 128

beta_one = 0.9
beta_two = 0.95
learn_rate = 0.02
adam_eps = 1e-08
norm_eps = 1e-06


def adam_update(summed, master, first, second, scale):
    clipped = summed * scale
    new_first = beta_one * first + (1.0 - beta_one) * clipped
    new_second = beta_two * second + (1.0 - beta_two) * clipped * clipped
    correct_one = 1.0 - beta_one**ADAM_STEP
    correct_two = 1.0 - beta_two**ADAM_STEP
    step_size = new_first / correct_one / (jnp.sqrt(new_second / correct_two) + adam_eps)
    new_master = master - learn_rate * step_size
    return (new_master, new_first, new_second)


def plain_body(replica_grads, master_weights, first_moment, second_moment, max_norm):
    groups = lax.axis_size("grp")
    shards = lax.axis_size("zero")
    local_grad = replica_grads[0]
    local_width = local_grad.shape[2]
    rows_dev = master_weights.shape[0]
    full_width = master_weights.shape[2]
    blocks = local_grad.reshape(groups, shards, rows_dev, 2, local_width)
    arrived = lax.all_to_all(
        lax.all_to_all(blocks[None], "grp", split_axis=1, concat_axis=0, tiled=True),
        "zero",
        split_axis=2,
        concat_axis=5,
        tiled=True,
    )
    summed = jnp.sum(arrived.astype(jnp.float32), axis=0)
    summed = summed.reshape(master_weights.shape)
    total = lax.psum(jnp.sum(summed * summed), ("grp", "zero"))
    scale = jnp.minimum(jnp.float32(1.0), max_norm[0] / (jnp.sqrt(total) + norm_eps))
    new_master, new_first, new_second = adam_update(
        summed, master_weights, first_moment, second_moment, scale
    )
    fresh = new_master.astype(jnp.bfloat16).reshape(1, 1, rows_dev, 2, full_width)
    own_tiles = lax.all_to_all(fresh, "zero", split_axis=4, concat_axis=1, tiled=True)
    tiled = lax.all_gather(own_tiles, "grp", axis=0, tiled=True)
    new_weights = tiled.reshape(groups * shards * rows_dev, 2, full_width // shards)
    return (new_master, new_first, new_second, new_weights)


def flip(index, mask, size):
    out = 0
    bit = 1
    while bit < size:
        b = (index // bit) % 2
        out = out + bit * ((1 - b) if mask & bit else b)
        bit *= 2
    return out


def greet(groups, shards, g, z):
    barrier = pltpu.get_barrier_semaphore()
    for k in range(1, shards):
        pl.semaphore_signal(barrier, inc=1, device_id=(g, flip(z, k, shards)), device_id_type=MESH)
    for j in range(1, groups):
        pl.semaphore_signal(barrier, inc=1, device_id=(flip(g, j, groups), z), device_id_type=MESH)
    pl.semaphore_wait(barrier, shards + groups - 2)


def remote(src, dst, send, recv, device):
    return pltpu.make_async_remote_copy(
        src_ref=src, dst_ref=dst, send_sem=send, recv_sem=recv,
        device_id=device, device_id_type=MESH,
    )


def scatter_kernel(groups, shards, grad, landed, norm, near, far, own, kept, pairs, got, sums, zone, gone,
                   f_send, f_recv, load_sem, p_send, p_recv, s_send, s_recv,
                   nz_send, nz_recv, ng_send, ng_recv, loc_sem):
    g, z = lax.axis_index("grp"), lax.axis_index("zero")
    gx, gy, diagonal = flip(g, 1, groups), flip(g, 2, groups), flip(g, 3, groups)
    first_to, second_to = (gx, gy), (gy, gx)
    rows = own.shape[2]
    order = list(range(shards - 1, -1, -1))

    def raw(k, h, d):
        block = diagonal if d else first_to[h]
        return remote(grad.at[block, flip(z, k, shards), h], (far if d else near).at[k, h],
                      f_send.at[k, h, d], f_recv.at[k, h, d], (first_to[h], z))

    def pair(k, h):
        return remote(pairs.at[k, h], got.at[k, h], p_send.at[k, h], p_recv.at[k, h], (second_to[h], z))

    def load(k, h, d):
        block = second_to[h] if d else g
        return pltpu.make_async_copy(grad.at[block, flip(z, k, shards), h], (kept if d else own).at[k, h],
                                     load_sem.at[k, h, d])

    def onward(k):
        return remote(sums.at[k], landed.at[z], s_send.at[k], s_recv.at[k], (g, flip(z, k, shards)))

    def begin(k):
        for d in (1, 0):
            for h in (0, 1):
                raw(k, h, d).start()

    for k in order:
        for d in (1, 0):
            for h in (0, 1):
                load(k, h, d).start()
    greet(groups, shards, g, z)
    ahead = 3
    for k in order[:ahead]:
        begin(k)
    stay = pltpu.make_async_copy(sums.at[0], landed.at[z], loc_sem)
    square = jnp.zeros(own.shape[3:], jnp.float32)
    for i in range(shards + 1):
        if i < shards:
            k = order[i]
            for h in (0, 1):
                load(k, h, 1).wait()
                raw(k, h, 1).wait_recv()

                def join(r, carry, k=k, h=h):
                    both = kept[k, h, r].astype(jnp.float32) + far[k, h, r].astype(jnp.float32)
                    pairs[k, h, r] = both.astype(jnp.bfloat16)
                    return carry

                lax.fori_loop(0, rows, join, 0)
                pair(k, h).start()
            if i + ahead < shards:
                begin(order[i + ahead])
        if i >= 1:
            k = order[i - 1]
            for h in (0, 1):
                load(k, h, 0).wait()
                raw(k, h, 0).wait_recv()
                pair(k, h).wait_recv()

                def add(r, acc, k=k, h=h):
                    total = own[k, h, r].astype(jnp.float32) + near[k, h, r].astype(jnp.float32)
                    total = total + got[k, h, r].astype(jnp.float32)
                    sums[k, h, r] = total.astype(jnp.bfloat16)
                    return acc + total * total

                square = lax.fori_loop(0, rows, add, square)
            if k:
                onward(k).start()
            else:
                stay.start()

    folded = square[0:8]
    for i in range(8, square.shape[0], 8):
        folded = folded + square[i:i + 8]
    zone[0] = folded

    def tell_zero(k):
        return remote(zone.at[0], zone.at[k], nz_send.at[k], nz_recv.at[k], (g, flip(z, k, shards)))

    def tell_group(j):
        return remote(gone.at[0], gone.at[j], ng_send.at[j], ng_recv.at[j], (flip(g, j, groups), z))

    for k in range(1, shards):
        tell_zero(k).start()
    for k in range(1, shards):
        tell_zero(k).wait_recv()
    gone[0] = jnp.sum(zone[...], axis=0)
    for j in range(1, groups):
        tell_group(j).start()
    for j in range(1, groups):
        tell_group(j).wait_recv()
    norm[...] = jnp.sum(gone[...], axis=0)

    for k in range(1, shards):
        tell_zero(k).wait_send()
    for j in range(1, groups):
        tell_group(j).wait_send()
    for k in order:
        for h in (0, 1):
            pair(k, h).wait_send()
            for d in (0, 1):
                raw(k, h, d).wait_send()
        if k:
            onward(k).wait()
        else:
            stay.wait()


def update_kernel(limit, norm, summed, master, first, second, out_master, out_first, out_second, fresh):
    total = jnp.full(master.shape[2:], jnp.sum(norm[...]), jnp.float32)
    scale = jnp.minimum(jnp.float32(1.0), limit[0] / (jnp.sqrt(total) + norm_eps))

    rate_one = learn_rate / (1.0 - beta_one**ADAM_STEP)
    over_two = 1.0 / (1.0 - beta_two**ADAM_STEP)

    def row(r, carry):
        for c in range(summed.shape[0]):
            clipped = summed[c, r].astype(jnp.float32) * scale
            new_first = beta_one * first[r, c] + (1.0 - beta_one) * clipped
            new_second = beta_two * second[r, c] + (1.0 - beta_two) * clipped * clipped
            below = jnp.sqrt(new_second * over_two) + adam_eps
            new_master = master[r, c] - new_first * rate_one / below
            out_master[r, c] = new_master
            out_first[r, c] = new_first
            out_second[r, c] = new_second
            fresh[c, r] = new_master.astype(jnp.bfloat16)
        return carry

    lax.fori_loop(0, master.shape[0], row, 0)


def gather_kernel(groups, shards, fresh, out, hold, z_send, z_recv, x_send, x_recv, y_send, y_recv,
                  u_send, u_recv, v_send, v_recv, loc_sem):
    g, z = lax.axis_index("grp"), lax.axis_index("zero")
    half = fresh.shape[1] // 2
    gx, gy = flip(g, 1, groups), flip(g, 2, groups)

    def spread(k):
        return remote(fresh.at[flip(z, k, shards)], out.at[g, z], z_send.at[k], z_recv.at[k],
                      (g, flip(z, k, shards)))

    def first_hop(k, send, recv, to):
        q = flip(z, k, shards)
        src = out.at[g, q] if k else fresh.at[z]
        return remote(src, out.at[g, q], send.at[k], recv.at[k], (to, z))

    def second_hop(k, origin, start, send, recv, to):
        q = flip(z, k, shards)
        ref = out.at[origin, q, pl.ds(start, half)]
        return remote(ref, ref, send.at[k], recv.at[k], (to, z))

    def hops(k):
        return (first_hop(k, x_send, x_recv, gx), first_hop(k, y_send, y_recv, gy))

    def turns(k):
        return (second_hop(k, gx, 0, u_send, u_recv, gy), second_hop(k, gy, half, v_send, v_recv, gx))

    load = pltpu.make_async_copy(fresh.at[z], hold, loc_sem.at[0])
    store = pltpu.make_async_copy(hold, out.at[g, z], loc_sem.at[1])
    load.start()
    greet(groups, shards, g, z)
    for k in range(1, shards):
        spread(k).start()
    lag = 1
    for s in range(shards + lag):
        if s < shards:
            if s:
                spread(s).wait_recv()
            for hop in hops(s):
                hop.start()
            if s == 0:
                load.wait()
                store.start()
        if s >= lag:
            for hop, turn in zip(hops(s - lag), turns(s - lag)):
                hop.wait_recv()
                turn.start()
    store.wait()
    for k in range(shards):
        if k:
            spread(k).wait_send()
        for hop in hops(k):
            hop.wait_send()
        for turn in turns(k):
            turn.wait()


def flat_body(replica_grads, master_weights, first_moment, second_moment, max_norm):
    groups = lax.axis_size("grp")
    shards = lax.axis_size("zero")
    rows = master_weights.shape[0]
    width = replica_grads.shape[3]
    tiles = width // LANES
    deep = 2 * tiles
    bf16, f32 = jnp.bfloat16, jnp.float32
    any_space = pl.BlockSpec(memory_space=pl.ANY)
    dma = pltpu.SemaphoreType.DMA
    limit = 60 * 1024 * 1024

    def keep(x, *order):
        return with_layout_constraint(x, Layout(major_to_minor=order))

    def flat(x):
        x = x.reshape(x.shape[0], 2, -1, LANES)
        return jnp.swapaxes(keep(x, 0, 2, 1, 3), 1, 2)

    grad = flat(replica_grads[0]).reshape(groups, shards, 2, rows // 2, deep, LANES)
    master, first, second = (
        flat(x).reshape(rows, shards, deep, LANES)
        for x in (master_weights, first_moment, second_moment)
    )

    piece = (rows, deep, LANES)
    halves = (shards, 2, rows // 2, deep, LANES)
    landed, norm = pl.pallas_call(
        functools.partial(scatter_kernel, groups, shards),
        out_shape=(
            jax.ShapeDtypeStruct(halves, bf16),
            jax.ShapeDtypeStruct((8, LANES), f32),
        ),
        in_specs=[any_space],
        out_specs=(any_space, pl.BlockSpec(memory_space=pltpu.VMEM)),
        scratch_shapes=[
            *[pltpu.VMEM(halves, bf16)] * 7,
            pltpu.VMEM((shards, 8, LANES), f32),
            pltpu.VMEM((groups, 8, LANES), f32),
            *[dma((shards, 2, 2))] * 3,
            *[dma((shards, 2))] * 2,
            *[dma((shards,))] * 4,
            dma((groups,)),
            dma((groups,)),
            dma,
        ],
        compiler_params=pltpu.CompilerParams(
            collective_id=0, has_side_effects=True, vmem_limit_bytes=limit
        ),
    )(grad)

    step = 8 if rows % 8 == 0 else 1
    by_row = pl.BlockSpec((step, shards, deep, LANES), lambda i: (i, 0, 0, 0))
    by_shard = pl.BlockSpec((shards, step, deep, LANES), lambda i: (0, i, 0, 0))
    state = jax.ShapeDtypeStruct((rows, shards, deep, LANES), f32)
    new_master, new_first, new_second, fresh = pl.pallas_call(
        update_kernel,
        grid=(rows // step,),
        out_shape=(state, state, state, jax.ShapeDtypeStruct((shards,) + piece, bf16)),
        in_specs=[
            pl.BlockSpec(memory_space=pltpu.SMEM),
            pl.BlockSpec((8, LANES), lambda i: (0, 0)),
            by_shard, by_row, by_row, by_row,
        ],
        out_specs=(by_row, by_row, by_row, by_shard),
        compiler_params=pltpu.CompilerParams(vmem_limit_bytes=limit),
    )(max_norm, norm, landed.reshape((shards,) + piece), master, first, second)

    gathered = pl.pallas_call(
        functools.partial(gather_kernel, groups, shards),
        out_shape=jax.ShapeDtypeStruct((groups, shards) + piece, bf16),
        in_specs=[any_space],
        out_specs=any_space,
        scratch_shapes=[pltpu.VMEM(piece, bf16)] + [dma((shards,))] * 10 + [dma((2,))],
        compiler_params=pltpu.CompilerParams(
            collective_id=1, has_side_effects=True, vmem_limit_bytes=limit
        ),
    )(fresh)

    def unflat(x, shape):
        x = x.reshape(shape[0], -1, 2, LANES)
        return keep(jnp.swapaxes(x, 1, 2), 0, 2, 1, 3).reshape(shape)

    shape = master_weights.shape
    return (
        unflat(new_master, shape),
        unflat(new_first, shape),
        unflat(new_second, shape),
        unflat(gathered, replica_grads.shape[1:]),
    )


def body(replica_grads, master_weights, first_moment, second_moment, max_norm):
    groups = lax.axis_size("grp")
    shards = lax.axis_size("zero")
    rows = master_weights.shape[0]
    width = replica_grads.shape[3]
    deep = 2 * width // LANES
    power = shards > 1 and shards & (shards - 1) == 0
    fits = groups * shards * rows * deep * LANES * 2 * 7 // 4 < 48 * 1024 * 1024
    whole = width % LANES == 0 and deep % 8 == 0 and rows % 2 == 0
    run = flat_body if groups == 4 and power and fits and whole else plain_body
    return run(replica_grads, master_weights, first_moment, second_moment, max_norm)


def solution(mesh):
    in_specs = (
        P("grp", None, None, "zero"),
        P(("grp", "zero"), None, None),
        P(("grp", "zero"), None, None),
        P(("grp", "zero"), None, None),
        P(),
    )
    out_specs = (
        P(("grp", "zero"), None, None),
        P(("grp", "zero"), None, None),
        P(("grp", "zero"), None, None),
        P(None, None, "zero"),
    )
    return jax.shard_map(body, mesh=mesh, in_specs=in_specs, out_specs=out_specs, check_vma=False)
```
